128 devices in a mesh: data: 1, tp: 2 (over core), ep: 64 (over z, y, x).
Axes of the slice: x: 4, y: 4, z: 4, core: 2. Of those that a mesh axis runs over, the one named last changes fastest.
Arguments:
- tokens: bfloat16 [24576, 2048], P(('data', 'ep', 'tp'))
- expert_ids: int32 [24576, 6], P(('data', 'ep', 'tp'))
- gate_vals: float32 [24576, 6], P(('data', 'ep', 'tp'))
- slot_ids: int32 [24576, 6], P(('data', 'ep', 'tp'))
- send_counts: int32 [128, 64], P(('data', 'ep', 'tp'))
- shared_w1: bfloat16 [2048, 2816], P(None, 'tp')
- shared_w3: bfloat16 [2048, 2816], P(None, 'tp')
- shared_w2: bfloat16 [2816, 2048], P('tp')
- expert_w1: bfloat16 [64, 2048, 1408], P('ep')
- expert_w3: bfloat16 [64, 2048, 1408], P('ep')
- expert_w2: bfloat16 [64, 1408, 2048], P('ep')
Outputs:
- output: bfloat16 [24576, 2048], P(('data', 'ep', 'tp'))
All inputs are finite; a program needn't handle non-finite values.
Results may differ from the reference program's by a relative error of at most 0.00129.
Values are sent between devices in bfloat16 or wider.
A program may use at most 1 GiB of HBM per device.

```python
import jax
import jax.numpy as jnp
from jax import lax

EP = 64
TP = 2
TOKENS_DEV = 192
D = 2048
FS = 2816
FF = 1408
EXPERTS = 64
TOP = 6
HOT = 8
CAP = 72

N_SRC = EP * TP
TOKENS = TOKENS_DEV * N_SRC


def draw_routing(route_key):
    key_hot, key_wts, key_perm = jax.random.split(route_key, 3)
    experts = jnp.arange(EXPERTS, dtype=jnp.int32)
    offset = jax.random.randint(key_hot, (), 0, EXPERTS, dtype=jnp.int32)
    is_hot = ((experts - offset) % EXPERTS) < HOT
    weights = jax.random.randint(key_wts, (N_SRC, EXPERTS), 1, 3, dtype=jnp.int32)
    cum_wts = jnp.cumsum(jnp.where(is_hot[None, :], 0, weights), axis=1)
    cold_total = TOKENS_DEV * TOP - HOT * CAP
    bounds = (cold_total * cum_wts) // cum_wts[:, -1:]
    prev_bounds = jnp.concatenate([jnp.zeros((N_SRC, 1), jnp.int32), bounds[:, :-1]], axis=1)
    counts = jnp.where(is_hot[None, :], CAP, bounds - prev_bounds).astype(jnp.int32)
    run_ends = jnp.cumsum(counts, axis=1)
    copy_pos = jnp.arange(TOKENS_DEV * TOP, dtype=jnp.int32)
    expert_of = jax.vmap(lambda end_row: jnp.searchsorted(end_row, copy_pos, side="right"))(run_ends).astype(jnp.int32)
    slot_of = copy_pos[None, :] - jnp.take_along_axis(run_ends - counts, expert_of, axis=1)
    expert_of = expert_of.reshape(N_SRC, TOP, TOKENS_DEV).transpose(0, 2, 1)
    slot_of = slot_of.reshape(N_SRC, TOP, TOKENS_DEV).transpose(0, 2, 1)
    tok_perms = jax.vmap(lambda perm_key: jax.random.permutation(perm_key, TOKENS_DEV))(jax.random.split(key_perm, N_SRC))
    expert_of = jnp.take_along_axis(expert_of, tok_perms[:, :, None], axis=1)
    slot_of = jnp.take_along_axis(slot_of, tok_perms[:, :, None], axis=1)
    return expert_of.reshape(TOKENS, TOP).astype(jnp.int32), slot_of.reshape(TOKENS, TOP).astype(jnp.int32), counts


def scaled_normal(weight_key, shape, fan_in):
    return (jax.random.normal(weight_key, shape, jnp.float32) * fan_in ** -0.5).astype(jnp.bfloat16)


def setup_inputs(seed: int = 0, part: int = 0) -> dict:
    base_key = jax.random.key(seed)
    part_key = jax.random.fold_in(base_key, part)
    key_x, key_gate, key_route = jax.random.split(part_key, 3)
    weight_keys = jax.random.split(jax.random.key(seed + 1), 6)
    tokens = jax.random.normal(key_x, (TOKENS, D), jnp.float32).astype(jnp.bfloat16)
    expert_ids, slot_ids, send_counts = draw_routing(key_route)
    gate_vals = jax.random.uniform(key_gate, (TOKENS, TOP), jnp.float32, 0.5, 1.5) * TOP ** -0.5
    return {
        "tokens": tokens,
        "expert_ids": expert_ids,
        "gate_vals": gate_vals,
        "slot_ids": slot_ids,
        "send_counts": send_counts,
        "shared_w1": scaled_normal(weight_keys[0], (D, FS), D),
        "shared_w3": scaled_normal(weight_keys[1], (D, FS), D),
        "shared_w2": scaled_normal(weight_keys[2], (FS, D), FS),
        "expert_w1": scaled_normal(weight_keys[3], (EXPERTS, D, FF), D),
        "expert_w3": scaled_normal(weight_keys[4], (EXPERTS, D, FF), D),
        "expert_w2": scaled_normal(weight_keys[5], (EXPERTS, FF, D), FF),
    }


def shared_block(tok_block, shared_w1, shared_w3, shared_w2):
    pre_gate = jnp.dot(tok_block, shared_w1, preferred_element_type=jnp.float32)
    pre_up = jnp.dot(tok_block, shared_w3, preferred_element_type=jnp.float32)
    hidden = (jax.nn.silu(pre_gate) * pre_up).astype(jnp.bfloat16)
    return jnp.dot(hidden, shared_w2, preferred_element_type=jnp.float32)


def reference(tokens, expert_ids, gate_vals, slot_ids, send_counts, shared_w1, shared_w3, shared_w2, expert_w1, expert_w3, expert_w2):
    tok_blocks = tokens.reshape(N_SRC, TOKENS_DEV, D)
    shared_out = lax.map(lambda tok_block: shared_block(tok_block, shared_w1, shared_w3, shared_w2), tok_blocks).reshape(TOKENS, D)
    src_ids = jnp.arange(TOKENS, dtype=jnp.int32) // TOKENS_DEV
    row_limit = send_counts[src_ids[:, None], expert_ids]
    kept_mask = (slot_ids >= 0) & (slot_ids < row_limit)
    n_rows = N_SRC * EXPERTS * CAP
    dest_row = jnp.where(kept_mask, (src_ids[:, None] * EXPERTS + expert_ids) * CAP + slot_ids, n_rows)
    copy_ids = jnp.arange(TOKENS * TOP, dtype=jnp.int32)
    owner_ids = jnp.full((n_rows,), TOKENS * TOP, jnp.int32).at[dest_row.reshape(-1)].set(copy_ids, mode="drop")
    owner_ids = owner_ids.reshape(N_SRC, EXPERTS, CAP).transpose(1, 0, 2).reshape(EXPERTS, N_SRC * CAP)
    flat_gates = gate_vals.reshape(-1)

    def expert_step(running, step_in):
        w_in, w_up, w_out, own_ids = step_in
        tok_of = own_ids // TOP
        expert_rows = jnp.take(tokens, tok_of, axis=0, mode="fill", fill_value=0)
        pre_gate = jnp.dot(expert_rows, w_in, preferred_element_type=jnp.float32)
        pre_up = jnp.dot(expert_rows, w_up, preferred_element_type=jnp.float32)
        hidden = (jax.nn.silu(pre_gate) * pre_up).astype(jnp.bfloat16)
        routed = jnp.dot(hidden, w_out, preferred_element_type=jnp.float32).astype(jnp.bfloat16)
        weight = jnp.take(flat_gates, own_ids, mode="fill", fill_value=0)
        running = running.at[tok_of].add(weight[:, None] * routed.astype(jnp.float32), mode="drop")
        return running, None

    routed_sum = lax.scan(expert_step, jnp.zeros((TOKENS, D), jnp.float32), (expert_w1, expert_w3, expert_w2, owner_ids))[0]
    return (tokens.astype(jnp.float32) + shared_out + routed_sum).astype(jnp.bfloat16)
```

```python
import functools

import jax
import jax.numpy as jnp
from jax import lax
from jax.experimental import pallas as pl
from jax.experimental.pallas import tpu as pltpu
from jax.sharding import PartitionSpec as P

CAP_FACTOR = 4
SIDE = 4
GROUPS = SIDE * SIDE
UNIT = 8
LAGS = (1, 4, 7)


def capacity_rows(n_tok, top_k, n_exp):
    return min(n_tok, ((CAP_FACTOR * n_tok * top_k // n_exp + 7) // 8) * 8)


def swiglu(rows, w1, w3, w2):
    gate = jnp.dot(rows, w1, preferred_element_type=jnp.float32)
    up = jnp.dot(rows, w3, preferred_element_type=jnp.float32)
    hidden = (jax.nn.silu(gate) * up).astype(jnp.bfloat16)
    return jnp.dot(hidden, w2, preferred_element_type=jnp.float32)


def bf16_parts(weights):
    parts, rest = [], weights
    for _ in range(3):
        part = lax.reduce_precision(rest, 8, 7)
        rest = rest - part
        parts.append(part.astype(jnp.bfloat16))
    return parts


def expert_kernel(n_items, rows, w1, w3, w2, hop1, hop2, out, in_buf, out_buf, load_sem, send_sem, recv_sem, own_sem):
    me = lax.axis_index("ep")
    coords = (lax.rem(me, SIDE), lax.rem(me // SIDE, SIDE), me // GROUPS)
    bufs = (out_buf, hop1, hop2, out)

    def part(color, phase, item, at):
        buf = bufs[phase]
        if phase == 0 and color == 2:
            return buf.at[item, at]
        if (phase == 0 and color == 1) or (phase == 1 and color == 1):
            return buf.at[item, :, at]
        return buf.at[item, :, :, at]

    def start(phase, item):
        for color in range(3):

            @pl.when(lax.rem(item, 3) == color)
            def _():
                axis = (color + phase) % 3
                mine, before = coords[axis], coords[(axis + 2) % 3]
                kept, own = own_sem.at[item, phase], out_buf.at[item]
                if phase == 0:
                    pltpu.make_async_copy(part(color, 0, item, mine), hop1.at[item, mine], kept).start()
                elif phase == 1:
                    pltpu.make_async_copy(part(color, 1, item, mine), own.at[0], kept).start()
                else:
                    pltpu.make_async_copy(own.at[0, :, mine], own.at[1, before], kept).start()
                    for e in range(1, SIDE):
                        src = lax.rem(before + e, SIDE)
                        pltpu.make_async_copy(hop2.at[item, src, :, mine], own.at[1, src], kept).start()
                for d in (1, 3, 2):
                    to = lax.rem(mine + d, SIDE)
                    chip = [to if axis == i else coords[i] for i in range(3)]

                    def send(src_ref, dst_ref):
                        pltpu.make_async_remote_copy(
                            src_ref=src_ref,
                            dst_ref=dst_ref,
                            send_sem=send_sem.at[item, phase, d - 1],
                            recv_sem=recv_sem.at[item, phase, d - 1],
                            device_id={"ep": (chip[2] * SIDE + chip[1]) * SIDE + chip[0]},
                            device_id_type=pl.DeviceIdType.MESH,
                        ).start()

                    if phase < 2:
                        send(part(color, phase, item, to), bufs[phase + 1].at[item, mine])
                    else:
                        send(own.at[0, :, to], out.at[item, mine, before])
                        for e in range(1, SIDE):
                            src = lax.rem(before + e, SIDE)
                            send(hop2.at[item, src, :, to], out.at[item, mine, src])

    def wait(phase, item):
        block = bufs[phase + 1].at[item, 0]
        pltpu.make_async_copy(block, block, own_sem.at[item, phase]).wait()
        for d in range(3):
            pltpu.make_async_remote_copy(
                src_ref=block,
                dst_ref=block,
                send_sem=send_sem.at[item, phase, d],
                recv_sem=recv_sem.at[item, phase, d],
                device_id={"ep": lax.rem(me + 1, GROUPS * SIDE)},
                device_id_type=pl.DeviceIdType.MESH,
            ).wait()

    def load(item, slot):
        return pltpu.make_async_copy(rows.at[:, pl.ds(item * UNIT, UNIT)], in_buf.at[slot], load_sem.at[slot])

    load(0, 0).start()

    def body(t, _):
        @pl.when(t < n_items)
        def _():
            slot = lax.rem(t, 2)

            @pl.when(t + 1 < n_items)
            def _():
                load(t + 1, 1 - slot).start()

            load(t, slot).wait()

        def exchange():
            for phase, lag in enumerate(LAGS):
                item = t - lag

                @pl.when((item >= 0) & (item < n_items))
                def _():
                    if phase > 0:
                        wait(phase - 1, item)
                    start(phase, item)

        @pl.when(t < n_items)
        def _():
            slot = lax.rem(t, 2)
            n_src, _, d_model = in_buf.shape[1:]
            x = in_buf[slot].astype(jnp.float32).reshape(n_src * UNIT, d_model).astype(jnp.bfloat16)
            gate = jnp.dot(x, w1[...], preferred_element_type=jnp.float32)
            up = jnp.dot(x, w3[...], preferred_element_type=jnp.float32)
            hidden = (gate * jax.nn.sigmoid(gate) * up).astype(jnp.bfloat16)
            exchange()
            res = jnp.dot(hidden, w2[...], preferred_element_type=jnp.float32)
            out_buf[t] = res.reshape(SIDE, SIDE, SIDE, UNIT, d_model).astype(jnp.bfloat16)

        @pl.when(t >= n_items)
        def _():
            exchange()

        return 0

    lax.fori_loop(0, n_items + LAGS[2], body, 0)

    def finish(item, _):
        wait(2, item)
        for color in range(3):

            @pl.when(lax.rem(item, 3) == color)
            def _():
                pltpu.make_async_copy(out_buf.at[item, 1], out.at[item, coords[(color + 2) % 3]], own_sem.at[item, 2]).start()

        return 0

    lax.fori_loop(0, n_items, finish, 0)

    def done(item, _):
        pltpu.make_async_copy(out_buf.at[item, 1], out.at[item, 0], own_sem.at[item, 2]).wait()
        return 0

    lax.fori_loop(0, n_items, done, 0)


def solution(mesh):
    ep_size = mesh.shape["ep"]
    row_spec = P(("data", "ep", "tp"), None)
    expert_spec = P("ep", None, None)

    def layer_body(tokens, expert_ids, gate_vals, slot_ids, send_counts, shared_w1, shared_w3, shared_w2, expert_w1, expert_w3, expert_w2):
        n_tok, d_model = tokens.shape
        top_k = expert_ids.shape[1]
        n_exp = ep_size
        d_ff = expert_w1.shape[2]
        cap = capacity_rows(n_tok, top_k, n_exp)
        n_rows = n_exp * cap
        swap = [(0, 1), (1, 0)]

        gathered = lax.all_gather(tokens, "ep", axis=0, tiled=True).reshape(ep_size, n_tok, d_model)

        is_exp = expert_ids[:, :, None] == jnp.arange(n_exp, dtype=jnp.int32)
        row_limit = jnp.sum(jnp.where(is_exp, send_counts[0], 0), axis=2)
        kept = (slot_ids >= 0) & (slot_ids < row_limit)
        is_slot = kept[:, :, None] & (slot_ids[:, :, None] == jnp.arange(cap, dtype=jnp.int32))
        tok_nums = jnp.arange(1, n_tok + 1, dtype=jnp.float32)[:, None, None]
        owners = jnp.einsum("tje,tjr->er", jnp.where(is_exp, tok_nums, 0.0).astype(jnp.bfloat16), is_slot.astype(jnp.bfloat16), preferred_element_type=jnp.float32)
        owners = lax.all_to_all(owners, "ep", 0, 0, tiled=True).astype(jnp.int32)
        other = lax.ppermute(tokens, "tp", swap)
        part = swiglu(jnp.concatenate([tokens, other], axis=0), shared_w1, shared_w3, shared_w2)
        shared_out = part[:n_tok] + lax.ppermute(part[n_tok:], "tp", swap)

        n_items = cap // UNIT
        item = slot_ids // UNIT
        ex, ey, ez = expert_ids % SIDE, expert_ids // SIDE % SIDE, expert_ids // GROUPS
        place = jnp.where(item % 3 == 0, (ez * SIDE + ey) * SIDE + ex, jnp.where(item % 3 == 1, (ex * SIDE + ez) * SIDE + ey, (ey * SIDE + ex) * SIDE + ez))
        dest = jnp.where(kept, (item * n_exp + place) * UNIT + slot_ids % UNIT, -1)
        row_nums = jnp.arange(n_rows, dtype=jnp.int32)
        weights = jnp.zeros((n_tok, n_rows), jnp.float32)
        for j in range(top_k):
            weights = weights + jnp.where(dest[:, j : j + 1] == row_nums[None, :], gate_vals[:, j : j + 1], 0.0)
        weights = lax.optimization_barrier(jnp.concatenate(bf16_parts(weights), axis=0))

        pick = owners.reshape(ep_size, cap)[:, :, None] == jnp.arange(1, n_tok + 1, dtype=jnp.int32)
        rows = jnp.einsum("srt,std->srd", pick.astype(jnp.bfloat16), gathered, preferred_element_type=jnp.float32).astype(jnp.bfloat16)
        vmem = pl.BlockSpec(memory_space=pltpu.VMEM)
        hbm = pl.BlockSpec(memory_space=pl.ANY)
        boxes = (n_items, SIDE, SIDE, SIDE, UNIT, d_model)
        back = pl.pallas_call(
            functools.partial(expert_kernel, n_items),
            name="expert_return",
            out_shape=[jax.ShapeDtypeStruct(boxes, jnp.bfloat16)] * 3,
            in_specs=[hbm, vmem, vmem, vmem],
            out_specs=[hbm] * 3,
            scratch_shapes=[
                pltpu.VMEM((2, ep_size, UNIT, d_model), jnp.bfloat16),
                pltpu.VMEM(boxes, jnp.bfloat16),
                pltpu.SemaphoreType.DMA((2,)),
                pltpu.SemaphoreType.DMA((n_items, 3, 3)),
                pltpu.SemaphoreType.DMA((n_items, 3, 3)),
                pltpu.SemaphoreType.DMA((n_items, 3)),
            ],
            compiler_params=pltpu.CompilerParams(has_side_effects=True, vmem_limit_bytes=66_000_000),
            cost_estimate=pl.CostEstimate(flops=6 * n_rows * d_model * d_ff, bytes_accessed=n_rows * d_model * 6, transcendentals=n_rows * d_ff),
        )(rows, expert_w1[0], expert_w3[0], expert_w2[0])[2].reshape(n_rows, d_model)
        routed = jnp.dot(weights, back, preferred_element_type=jnp.float32)
        routed = routed[:n_tok] + routed[n_tok : 2 * n_tok] + routed[2 * n_tok :]
        return (tokens.astype(jnp.float32) + shared_out + routed).astype(jnp.bfloat16)

    return jax.shard_map(
        layer_body,
        mesh=mesh,
        in_specs=(row_spec, row_spec, row_spec, row_spec, row_spec, P(None, "tp"), P(None, "tp"), P("tp", None), expert_spec, expert_spec, expert_spec),
        out_specs=row_spec,
        check_vma=False,
    )
```

```python
import functools

import jax
import jax.numpy as jnp
from jax import lax
from jax.experimental import pallas as pl
from jax.experimental.pallas import tpu as pltpu
from jax.sharding import PartitionSpec as P

CAP_FACTOR = 4
SIDE = 4
GROUPS = SIDE * SIDE
UNIT = 8
LAGS = (0, 2, 4, 5, 6, 9, 12)


def capacity_rows(n_tok, top_k, n_exp):
    return min(n_tok, ((CAP_FACTOR * n_tok * top_k // n_exp + 7) // 8) * 8)


def swiglu(rows, w1, w3, w2):
    gate = jnp.dot(rows, w1, preferred_element_type=jnp.float32)
    up = jnp.dot(rows, w3, preferred_element_type=jnp.float32)
    hidden = (jax.nn.silu(gate) * up).astype(jnp.bfloat16)
    return jnp.dot(hidden, w2, preferred_element_type=jnp.float32)


def bf16_parts(weights):
    parts, rest = [], weights
    for _ in range(3):
        part = lax.reduce_precision(rest, 8, 7)
        rest = rest - part
        parts.append(part.astype(jnp.bfloat16))
    return parts


def expert_kernel(n_items, packed, w1, w3, w2, out1, out2, came, back1, back2, back, in_buf, out_buf, load_sem, send_sem, recv_sem, own_sem):
    me = lax.axis_index("ep")
    coords = (lax.rem(me, SIDE), lax.rem(me // SIDE, SIDE), me // GROUPS)
    away, home = (packed, out1, out2, came), (out_buf, back1, back2, back)

    def start(way, phase, item):
        bufs = (away, home)[way]
        for color in range(3):

            @pl.when(lax.rem(item, 3) == color)
            def _():
                axis = (color + phase) % 3
                mine, before = coords[axis], coords[(axis + 2) % 3]
                kept, own = own_sem.at[way, item, phase], out_buf.at[item]
                if phase == 0:
                    pieces = [(lambda at: bufs[0].at[item, :, :, at], None)]
                elif way == 1 and phase == 1:
                    pieces = [(lambda at: bufs[1].at[item, :, :, at], None)]
                else:
                    held = own.at[phase - 1 - way]
                    pieces = [(lambda at, held=held: held.at[:, at], before)]
                    for e in range(1, SIDE):
                        src = lax.rem(before + e, SIDE)
                        pieces.append((lambda at, src=src: bufs[phase].at[item, src, :, at], src))
                if way == 1 and phase == 0:
                    stay = bufs[1].at[item, mine]
                else:
                    stay = own.at[phase - way]
                for piece, place in pieces:
                    pltpu.make_async_copy(piece(mine), stay if place is None else stay.at[place], kept).start()
                for d in (1, 3, 2):
                    to = lax.rem(mine + d, SIDE)
                    chip = [to if axis == i else coords[i] for i in range(3)]
                    for piece, place in pieces:
                        box = bufs[phase + 1].at[item, mine]
                        pltpu.make_async_remote_copy(
                            src_ref=piece(to),
                            dst_ref=box if place is None else box.at[place],
                            send_sem=send_sem.at[way, item, phase, d - 1],
                            recv_sem=recv_sem.at[way, item, phase, d - 1],
                            device_id={"ep": (chip[2] * SIDE + chip[1]) * SIDE + chip[0]},
                            device_id_type=pl.DeviceIdType.MESH,
                        ).start()

    def wait(way, phase, item):
        block = (away, home)[way][phase + 1].at[item, 0]
        pltpu.make_async_copy(block, block, own_sem.at[way, item, phase]).wait()
        for d in range(3):
            pltpu.make_async_remote_copy(
                src_ref=block,
                dst_ref=block,
                send_sem=send_sem.at[way, item, phase, d],
                recv_sem=recv_sem.at[way, item, phase, d],
                device_id={"ep": lax.rem(me + 1, GROUPS * SIDE)},
                device_id_type=pl.DeviceIdType.MESH,
            ).wait()

    def load(item, slot):
        for color in range(3):

            @pl.when(lax.rem(item, 3) == color)
            def _():
                mine = coords[(color + 2) % 3]
                pltpu.make_async_copy(out_buf.at[item, 2], in_buf.at[slot, mine], load_sem.at[slot]).start()
                for e in range(1, SIDE):
                    src = lax.rem(mine + e, SIDE)
                    pltpu.make_async_copy(came.at[item, src], in_buf.at[slot, src], load_sem.at[slot]).start()

    def first(item, _):
        start(0, 0, item)
        return 0

    lax.fori_loop(0, n_items, first, 0)

    def at_step(t, lag, act):
        item = t - lag

        @pl.when((item >= 0) & (item < n_items))
        def _():
            act(item)

    def body(t, _):
        def middle(item):
            wait(0, 0, item)
            start(0, 1, item)

        def arrive(item):
            wait(0, 1, item)
            start(0, 2, item)

        def fetch(item):
            wait(0, 2, item)
            load(item, lax.rem(item, 2))

        at_step(t, LAGS[0], middle)
        at_step(t, LAGS[1], arrive)
        at_step(t, LAGS[2], fetch)

        def exchange():
            for phase in range(3):

                def go(item, phase=phase):
                    if phase > 0:
                        wait(1, phase - 1, item)
                    start(1, phase, item)

                at_step(t, LAGS[4 + phase], go)

        now = t - LAGS[3]
        busy = (now >= 0) & (now < n_items)

        @pl.when(busy)
        def _():
            slot = lax.rem(now, 2)
            d_model = in_buf.shape[-1]
            pltpu.make_async_copy(came.at[now], in_buf.at[slot], load_sem.at[slot]).wait()
            x = in_buf[slot].astype(jnp.float32).reshape(SIDE**3 * UNIT, d_model).astype(jnp.bfloat16)
            gate = jnp.dot(x, w1[...], preferred_element_type=jnp.float32)
            up = jnp.dot(x, w3[...], preferred_element_type=jnp.float32)
            hidden = (gate * jax.nn.sigmoid(gate) * up).astype(jnp.bfloat16)
            exchange()
            res = jnp.dot(hidden, w2[...], preferred_element_type=jnp.float32)
            out_buf[now] = res.reshape(SIDE, SIDE, SIDE, UNIT, d_model).astype(jnp.bfloat16)

        @pl.when(jnp.logical_not(busy))
        def _():
            exchange()

        return 0

    lax.fori_loop(0, n_items + LAGS[6], body, 0)

    def finish(item, _):
        wait(1, 2, item)
        for color in range(3):

            @pl.when(lax.rem(item, 3) == color)
            def _():
                pltpu.make_async_copy(out_buf.at[item, 1], back.at[item, coords[(color + 2) % 3]], own_sem.at[1, item, 2]).start()

        return 0

    lax.fori_loop(0, n_items, finish, 0)

    def done(item, _):
        pltpu.make_async_copy(out_buf.at[item, 1], back.at[item, 0], own_sem.at[1, item, 2]).wait()
        return 0

    lax.fori_loop(0, n_items, done, 0)


def solution(mesh):
    ep_size = mesh.shape["ep"]
    row_spec = P(("data", "ep", "tp"), None)
    expert_spec = P("ep", None, None)

    def layer_body(tokens, expert_ids, gate_vals, slot_ids, send_counts, shared_w1, shared_w3, shared_w2, expert_w1, expert_w3, expert_w2):
        n_tok, d_model = tokens.shape
        top_k = expert_ids.shape[1]
        n_exp = ep_size
        d_ff = expert_w1.shape[2]
        cap = capacity_rows(n_tok, top_k, n_exp)
        n_rows = n_exp * cap
        swap = [(0, 1), (1, 0)]

        is_exp = expert_ids[:, :, None] == jnp.arange(n_exp, dtype=jnp.int32)
        row_limit = jnp.sum(jnp.where(is_exp, send_counts[0], 0), axis=2)
        kept = (slot_ids >= 0) & (slot_ids < row_limit)

        other = lax.ppermute(tokens, "tp", swap)
        part = swiglu(jnp.concatenate([tokens, other], axis=0), shared_w1, shared_w3, shared_w2)
        shared_out = part[:n_tok] + lax.ppermute(part[n_tok:], "tp", swap)

        n_items = cap // UNIT
        item = slot_ids // UNIT
        ex, ey, ez = expert_ids % SIDE, expert_ids // SIDE % SIDE, expert_ids // GROUPS
        place = jnp.where(item % 3 == 0, (ez * SIDE + ey) * SIDE + ex, jnp.where(item % 3 == 1, (ex * SIDE + ez) * SIDE + ey, (ey * SIDE + ex) * SIDE + ez))
        dest = jnp.where(kept, (item * n_exp + place) * UNIT + slot_ids % UNIT, -1)
        row_nums = jnp.arange(n_rows, dtype=jnp.int32)
        weights = jnp.zeros((n_tok, n_rows), jnp.float32)
        sel = jnp.zeros((n_tok, n_rows), jnp.bool_)
        for j in range(top_k):
            here = dest[:, j : j + 1] == row_nums[None, :]
            sel = sel | here
            weights = weights + jnp.where(here, gate_vals[:, j : j + 1], 0.0)
        weights = lax.optimization_barrier(jnp.concatenate(bf16_parts(weights), axis=0))

        boxes = (n_items, SIDE, SIDE, SIDE, UNIT, d_model)
        packed = lax.dot_general(sel.astype(jnp.bfloat16), tokens, (((0,), (0,)), ((), ())), preferred_element_type=jnp.float32)
        packed = packed.astype(jnp.bfloat16).reshape(boxes)
        vmem = pl.BlockSpec(memory_space=pltpu.VMEM)
        hbm = pl.BlockSpec(memory_space=pl.ANY)
        back = pl.pallas_call(
            functools.partial(expert_kernel, n_items),
            name="expert_exchange",
            out_shape=[jax.ShapeDtypeStruct(boxes, jnp.bfloat16)] * 6,
            in_specs=[hbm, vmem, vmem, vmem],
            out_specs=[hbm] * 6,
            scratch_shapes=[
                pltpu.VMEM((2,) + boxes[1:], jnp.bfloat16),
                pltpu.VMEM(boxes, jnp.bfloat16),
                pltpu.SemaphoreType.DMA((2,)),
                pltpu.SemaphoreType.DMA((2, n_items, 3, 3)),
                pltpu.SemaphoreType.DMA((2, n_items, 3, 3)),
                pltpu.SemaphoreType.DMA((2, n_items, 3)),
            ],
            compiler_params=pltpu.CompilerParams(has_side_effects=True, vmem_limit_bytes=66_000_000),
            cost_estimate=pl.CostEstimate(flops=6 * n_rows * d_model * d_ff, bytes_accessed=n_rows * d_model * 6, transcendentals=n_rows * d_ff),
        )(packed, expert_w1[0], expert_w3[0], expert_w2[0])[5].reshape(n_rows, d_model)
        routed = jnp.dot(weights, back, preferred_element_type=jnp.float32)
        routed = routed[:n_tok] + routed[n_tok : 2 * n_tok] + routed[2 * n_tok :]
        return (tokens.astype(jnp.float32) + shared_out + routed).astype(jnp.bfloat16)

    return jax.shard_map(
        layer_body,
        mesh=mesh,
        in_specs=(row_spec, row_spec, row_spec, row_spec, row_spec, P(None, "tp"), P(None, "tp"), P("tp", None), expert_spec, expert_spec, expert_spec),
        out_specs=row_spec,
        check_vma=False,
    )
```

```python
import functools

import jax
import jax.numpy as jnp
from jax import lax
from jax.experimental import pallas as pl
from jax.experimental.pallas import tpu as pltpu
from jax.sharding import PartitionSpec as P

CAP_FACTOR = 4
SIDE = 4
GROUPS = SIDE * SIDE
UNIT = 8
LAGS = (0, 3, 5, 6, 7, 9, 11)


def capacity_rows(n_tok, top_k, n_exp):
    return min(n_tok, ((CAP_FACTOR * n_tok * top_k // n_exp + 7) // 8) * 8)


def swiglu(rows, w1, w3, w2):
    gate = jnp.dot(rows, w1, preferred_element_type=jnp.float32)
    up = jnp.dot(rows, w3, preferred_element_type=jnp.float32)
    hidden = (jax.nn.silu(gate) * up).astype(jnp.bfloat16)
    return jnp.dot(hidden, w2, preferred_element_type=jnp.float32)


def bf16_parts(weights):
    parts, rest = [], weights
    for _ in range(3):
        part = lax.reduce_precision(rest, 8, 7)
        rest = rest - part
        parts.append(part.astype(jnp.bfloat16))
    return parts


def expert_kernel(n_items, toks, dest, w1_hbm, w3_hbm, w2_hbm, out1, out2, came, back1, back2, back, in_buf, out_buf, w1, w3, w2, load_sem, send_sem, recv_sem, own_sem, weight_sem):
    me = lax.axis_index("ep")
    coords = (lax.rem(me, SIDE), lax.rem(me // SIDE, SIDE), me // GROUPS)
    away, home = (out_buf, out1, out2, came), (out_buf, back1, back2, back)

    def start(way, phase, item):
        bufs = (away, home)[way]
        for color in range(3):

            @pl.when(lax.rem(item, 3) == color)
            def _():
                axis = (color + phase) % 3
                mine, before = coords[axis], coords[(axis + 2) % 3]
                kept, own = own_sem.at[way, item, phase], out_buf.at[item]
                if phase < 2:
                    pieces = [(lambda at: bufs[phase].at[item, :, :, at], None)]
                else:
                    held = own.at[0]
                    pieces = [(lambda at, held=held: held.at[:, at], before)]
                    for e in range(1, SIDE):
                        src = lax.rem(before + e, SIDE)
                        pieces.append((lambda at, src=src: bufs[phase].at[item, src, :, at], src))
                stay = bufs[1].at[item, mine] if phase == 0 else own.at[phase - 1]
                for piece, place in pieces:
                    pltpu.make_async_copy(piece(mine), stay if place is None else stay.at[place], kept).start()
                for d in (1, 3, 2):
                    to = lax.rem(mine + d, SIDE)
                    chip = [to if axis == i else coords[i] for i in range(3)]
                    for piece, place in pieces:
                        box = bufs[phase + 1].at[item, mine]
                        pltpu.make_async_remote_copy(
                            src_ref=piece(to),
                            dst_ref=box if place is None else box.at[place],
                            send_sem=send_sem.at[way, item, phase, d - 1],
                            recv_sem=recv_sem.at[way, item, phase, d - 1],
                            device_id={"ep": (chip[2] * SIDE + chip[1]) * SIDE + chip[0]},
                            device_id_type=pl.DeviceIdType.MESH,
                        ).start()

    def wait(way, phase, item):
        block = (away, home)[way][phase + 1].at[item, 0]
        pltpu.make_async_copy(block, block, own_sem.at[way, item, phase]).wait()
        for d in range(3):
            pltpu.make_async_remote_copy(
                src_ref=block,
                dst_ref=block,
                send_sem=send_sem.at[way, item, phase, d],
                recv_sem=recv_sem.at[way, item, phase, d],
                device_id={"ep": lax.rem(me + 1, GROUPS * SIDE)},
                device_id_type=pl.DeviceIdType.MESH,
            ).wait()

    def load(item, slot):
        for color in range(3):

            @pl.when(lax.rem(item, 3) == color)
            def _():
                mine = coords[(color + 2) % 3]
                pltpu.make_async_copy(out_buf.at[item, 1], in_buf.at[slot, mine], load_sem.at[slot]).start()
                for e in range(1, SIDE):
                    src = lax.rem(mine + e, SIDE)
                    pltpu.make_async_copy(came.at[item, src], in_buf.at[slot, src], load_sem.at[slot]).start()

    weights = [pltpu.make_async_copy(src, dst, weight_sem.at[i]) for i, (src, dst) in enumerate(((w1_hbm, w1), (w3_hbm, w3), (w2_hbm, w2)))]
    for copy in weights:
        copy.start()

    n_tok, d_model = toks.shape
    per_item = SIDE**3 * UNIT

    def first(t, _):
        @pl.when(t < n_items)
        def _():
            row_nums = lax.broadcasted_iota(jnp.int32, (n_tok, per_item), 1) + t * per_item
            sel = jnp.zeros((n_tok, per_item), jnp.float32)
            for j in range(dest.shape[1]):
                sel = jnp.where(dest[:, j : j + 1] == row_nums, 1.0, sel)
            res = lax.dot_general(sel.astype(jnp.bfloat16), toks[...], (((0,), (0,)), ((), ())), preferred_element_type=jnp.float32)
            out_buf[t] = res.reshape(SIDE, SIDE, SIDE, UNIT, d_model).astype(jnp.bfloat16)

        @pl.when(t > 0)
        def _():
            start(0, 0, t - 1)

        return 0

    lax.fori_loop(0, n_items + 1, first, 0)
    for copy in weights:
        copy.wait()

    def at_step(t, lag, act):
        item = t - lag

        @pl.when((item >= 0) & (item < n_items))
        def _():
            act(item)

    def body(t, _):
        def middle(item):
            wait(0, 0, item)
            start(0, 1, item)

        def arrive(item):
            wait(0, 1, item)
            start(0, 2, item)

        def fetch(item):
            wait(0, 2, item)
            load(item, lax.rem(item, 2))

        at_step(t, LAGS[0], middle)
        at_step(t, LAGS[1], arrive)
        at_step(t, LAGS[2], fetch)

        def exchange():
            for phase in range(3):

                def go(item, phase=phase):
                    if phase > 0:
                        wait(1, phase - 1, item)
                    start(1, phase, item)

                at_step(t, LAGS[4 + phase], go)

        now = t - LAGS[3]
        busy = (now >= 0) & (now < n_items)

        @pl.when(busy)
        def _():
            slot = lax.rem(now, 2)
            pltpu.make_async_copy(came.at[now], in_buf.at[slot], load_sem.at[slot]).wait()
            x = in_buf[slot].astype(jnp.float32).reshape(SIDE**3 * UNIT, d_model).astype(jnp.bfloat16)
            gate = jnp.dot(x, w1[...], preferred_element_type=jnp.float32)
            up = jnp.dot(x, w3[...], preferred_element_type=jnp.float32)
            hidden = (gate * jax.nn.sigmoid(gate) * up).astype(jnp.bfloat16)
            exchange()
            res = jnp.dot(hidden, w2[...], preferred_element_type=jnp.float32)
            out_buf[now] = res.reshape(SIDE, SIDE, SIDE, UNIT, d_model).astype(jnp.bfloat16)

        @pl.when(jnp.logical_not(busy))
        def _():
            exchange()

        return 0

    lax.fori_loop(0, n_items + LAGS[6], body, 0)

    def finish(item, _):
        wait(1, 2, item)
        for color in range(3):

            @pl.when(lax.rem(item, 3) == color)
            def _():
                pltpu.make_async_copy(out_buf.at[item, 1], back.at[item, coords[(color + 2) % 3]], own_sem.at[1, item, 2]).start()

        return 0

    lax.fori_loop(0, n_items, finish, 0)

    def done(item, _):
        pltpu.make_async_copy(out_buf.at[item, 1], back.at[item, 0], own_sem.at[1, item, 2]).wait()
        return 0

    lax.fori_loop(0, n_items, done, 0)


def solution(mesh):
    ep_size = mesh.shape["ep"]
    row_spec = P(("data", "ep", "tp"), None)
    expert_spec = P("ep", None, None)

    def layer_body(tokens, expert_ids, gate_vals, slot_ids, send_counts, shared_w1, shared_w3, shared_w2, expert_w1, expert_w3, expert_w2):
        n_tok, d_model = tokens.shape
        top_k = expert_ids.shape[1]
        n_exp = ep_size
        d_ff = expert_w1.shape[2]
        cap = capacity_rows(n_tok, top_k, n_exp)
        n_rows = n_exp * cap
        swap = [(0, 1), (1, 0)]

        is_exp = expert_ids[:, :, None] == jnp.arange(n_exp, dtype=jnp.int32)
        row_limit = jnp.sum(jnp.where(is_exp, send_counts[0], 0), axis=2)
        kept = (slot_ids >= 0) & (slot_ids < row_limit)

        other = lax.ppermute(tokens, "tp", swap)
        part = swiglu(jnp.concatenate([tokens, other], axis=0), shared_w1, shared_w3, shared_w2)
        shared_out = part[:n_tok] + lax.ppermute(part[n_tok:], "tp", swap)

        n_items = cap // UNIT
        item = slot_ids // UNIT
        ex, ey, ez = expert_ids % SIDE, expert_ids // SIDE % SIDE, expert_ids // GROUPS
        place = jnp.where(item % 3 == 0, (ez * SIDE + ey) * SIDE + ex, jnp.where(item % 3 == 1, (ex * SIDE + ez) * SIDE + ey, (ey * SIDE + ex) * SIDE + ez))
        dest = jnp.where(kept, (item * n_exp + place) * UNIT + slot_ids % UNIT, -1)
        row_nums = jnp.arange(n_rows, dtype=jnp.int32)
        weights = jnp.zeros((n_tok, n_rows), jnp.float32)
        for j in range(top_k):
            weights = weights + jnp.where(dest[:, j : j + 1] == row_nums[None, :], gate_vals[:, j : j + 1], 0.0)
        weights = lax.optimization_barrier(jnp.concatenate(bf16_parts(weights), axis=0))

        boxes = (n_items, SIDE, SIDE, SIDE, UNIT, d_model)
        vmem = pl.BlockSpec(memory_space=pltpu.VMEM)
        hbm = pl.BlockSpec(memory_space=pl.ANY)
        back = pl.pallas_call(
            functools.partial(expert_kernel, n_items),
            name="expert_exchange",
            out_shape=[jax.ShapeDtypeStruct(boxes, jnp.bfloat16)] * 6,
            in_specs=[vmem, vmem, hbm, hbm, hbm],
            out_specs=[hbm] * 6,
            scratch_shapes=[
                pltpu.VMEM((2,) + boxes[1:], jnp.bfloat16),
                pltpu.VMEM(boxes, jnp.bfloat16),
                pltpu.VMEM((d_model, d_ff), jnp.bfloat16),
                pltpu.VMEM((d_model, d_ff), jnp.bfloat16),
                pltpu.VMEM((d_ff, d_model), jnp.bfloat16),
                pltpu.SemaphoreType.DMA((2,)),
                pltpu.SemaphoreType.DMA((2, n_items, 3, 3)),
                pltpu.SemaphoreType.DMA((2, n_items, 3, 3)),
                pltpu.SemaphoreType.DMA((2, n_items, 3)),
                pltpu.SemaphoreType.DMA((3,)),
            ],
            compiler_params=pltpu.CompilerParams(has_side_effects=True, vmem_limit_bytes=66_000_000),
            cost_estimate=pl.CostEstimate(flops=6 * n_rows * d_model * d_ff, bytes_accessed=n_rows * d_model * 6, transcendentals=n_rows * d_ff),
        )(tokens, dest, expert_w1[0], expert_w3[0], expert_w2[0])[5].reshape(n_rows, d_model)
        routed = jnp.dot(weights, back, preferred_element_type=jnp.float32)
        routed = routed[:n_tok] + routed[n_tok : 2 * n_tok] + routed[2 * n_tok :]
        return (tokens.astype(jnp.float32) + shared_out + routed).astype(jnp.bfloat16)

    return jax.shard_map(
        layer_body,
        mesh=mesh,
        in_specs=(row_spec, row_spec, row_spec, row_spec, row_spec, P(None, "tp"), P(None, "tp"), P("tp", None), expert_spec, expert_spec, expert_spec),
        out_specs=row_spec,
        check_vma=False,
    )
```
